32 devices in a mesh: face: 8 (over z, y), col: 4 (over x, core).
Axes of the slice: x: 2, y: 2, z: 4, core: 2. Of those that a mesh axis runs over, the one named last changes fastest.
Arguments:
- fields: float32 [4, 160, 80, 128], P(None, 'face', 'col'), may hold values from -6 to 6
- metric_diag: float32 [2, 160, 80], P(None, 'face', 'col'), may hold values from 0.05 to 0.5
- metric_cross: float32 [160, 80], P('face', 'col'), may hold values from -0.1 to 0.1
- point_mass: float32 [160, 80], P('face', 'col'), may hold values from 0.5 to 2
Outputs:
- biharmonic: float32 [4, 160, 80, 128], P(None, 'face', 'col')
The draws below stay inside these ranges and needn't reach their ends.
All inputs are finite; a program needn't handle non-finite values.
Results may differ from the reference program's by a relative error of at most 0.00024.
Values sent between devices are 32-bit elements; how exact they have to be, the bound alone decides.
A program may use at most 64 MiB of HBM per device.

```python
import math
import jax
import jax.numpy as jnp
import numpy as np
from jax import lax

FIELDS = 4
LEV = 128
NXP = 160
NYP = 80


def block_levels(key, shape, split, low, top_value):
    loudness = 1.0
    for axis_at, blocks in split:
        steps = jax.random.uniform(jax.random.fold_in(jax.random.fold_in(key, 6), axis_at), (blocks,), jnp.float32, low / len(split), top_value / len(split))
        loudness = loudness * jnp.repeat(jnp.exp(steps), shape[axis_at] // blocks).reshape((-1,) + (1,) * (len(shape) - 1 - axis_at))
    return loudness


def noise(own_key, shape, scale, bound, pieces=(), held_as=jnp.bfloat16):
    factor_of = block_levels(own_key, shape, pieces, -0.22, 0.18) if pieces else 1.0
    result = jax.random.normal(own_key, shape, jnp.float32) * scale * factor_of
    return jnp.minimum(jnp.maximum(result, -bound), bound).astype(held_as)


def setup_inputs(seed: int = 0) -> dict:
    key_list = jax.random.split(jax.random.key(seed), 5)
    fields = noise(key_list[0], (FIELDS, NXP, NYP, LEV), 1.0, 6.0, ((1, 8), (2, 4)), jnp.float32)
    metric_diag = jnp.clip(jnp.exp(math.log(0.5) - 2.3025851 * jax.random.uniform(key_list[1], (2, NXP, NYP), jnp.float32) ** block_levels(key_list[1], (2, NXP, NYP), ((1, 8), (2, 4)), -0.2, 0.2)), 0.05, 0.5)
    metric_cross = jnp.clip(jax.random.uniform(key_list[2], (NXP, NYP), jnp.float32, -0.1, 0.1) * block_levels(key_list[2], (NXP, NYP), ((0, 8), (1, 4)), -0.4, 0.0), -0.1, 0.1)
    point_mass = jnp.clip(jnp.exp(math.log(2.0) - 1.3862944 * jax.random.uniform(key_list[3], (NXP, NYP), jnp.float32) ** block_levels(key_list[3], (NXP, NYP), ((0, 8), (1, 4)), -0.2, 0.2)), 0.5, 2.0)
    return dict(fields=fields, metric_diag=metric_diag, metric_cross=metric_cross, point_mass=point_mass)


def derivative_table():
    small = 1.0 / np.sqrt(5.0)
    nodes = np.array([-1.0, -small, small, 1.0])
    count = nodes.shape[0]
    weights = np.array([np.prod([nodes[a] - nodes[k] for k in range(count) if k != a]) for a in range(count)])
    table = np.zeros((count, count))
    for a in range(count):
        for b in range(count):
            if a == b:
                table[a, b] = np.sum([1.0 / (nodes[a] - nodes[k]) for k in range(count) if k != a])
            else:
                table[a, b] = weights[a] / weights[b] / (nodes[a] - nodes[b])
    return jnp.asarray(table, jnp.float32)

def laplace(values, metric_diag, metric_cross):
    table = derivative_table()
    nfield, rows, cols, nlev = values.shape
    blocks_x = rows // 4
    blocks_y = cols // 4
    shaped = values.reshape(nfield, blocks_x, 4, blocks_y, 4, nlev)
    first_diag = metric_diag[0].reshape(1, blocks_x, 4, blocks_y, 4, 1)
    second_diag = metric_diag[1].reshape(1, blocks_x, 4, blocks_y, 4, 1)
    cross_term = metric_cross.reshape(1, blocks_x, 4, blocks_y, 4, 1)
    high = lax.Precision.HIGHEST
    grad_x = jnp.einsum('ab,febgcl->feagcl', table, shaped, precision=high)
    grad_y = jnp.einsum('cd,febgdl->febgcl', table, shaped, precision=high)
    flux_x = first_diag * grad_x + cross_term * grad_y
    flux_y = cross_term * grad_x + second_diag * grad_y
    weak = jnp.einsum('ba,febgcl->feagcl', table, flux_x, precision=high)
    weak = weak + jnp.einsum('dc,febgdl->febgcl', table, flux_y, precision=high)
    return (-weak).reshape(nfield, rows, cols, nlev)

def assemble(padded):
    rows = padded.shape[1] - 2
    cols = padded.shape[2] - 2
    row_local = jnp.arange(rows, dtype=jnp.int32) % 4
    col_local = jnp.arange(cols, dtype=jnp.int32) % 4
    row_low = (row_local == 0).astype(jnp.float32).reshape(1, rows, 1, 1)
    row_high = (row_local == 3).astype(jnp.float32).reshape(1, rows, 1, 1)
    col_low = (col_local == 0).astype(jnp.float32).reshape(1, 1, cols, 1)
    col_high = (col_local == 3).astype(jnp.float32).reshape(1, 1, cols, 1)
    summed = padded[:, 1:-1] + row_low * padded[:, :-2] + row_high * padded[:, 2:]
    return summed[:, :, 1:-1] + col_low * summed[:, :, :-2] + col_high * summed[:, :, 2:]

def wrap_pad(values):
    return jnp.pad(values, ((0, 0), (1, 1), (1, 1), (0, 0)), mode='wrap')

def reference(fields, metric_diag, metric_cross, point_mass):
    mass_sum = assemble(wrap_pad(point_mass[None, :, :, None]))
    first = assemble(wrap_pad(laplace(fields, metric_diag, metric_cross))) / mass_sum
    return assemble(wrap_pad(laplace(first, metric_diag, metric_cross))) / mass_sum
```

```python
import functools

import jax
import jax.numpy as jnp
import numpy as np
from jax import lax
from jax.experimental import pallas as pl
from jax.experimental.pallas import tpu as pltpu
from jax.sharding import PartitionSpec as P

MESH = pl.DeviceIdType.MESH


def derivative_table():
    small = 1.0 / np.sqrt(5.0)
    nodes = np.array([-1.0, -small, small, 1.0])
    count = nodes.shape[0]
    weights = np.array(
        [np.prod([nodes[a] - nodes[k] for k in range(count) if k != a]) for a in range(count)]
    )
    table = np.zeros((count, count))
    for a in range(count):
        for b in range(count):
            if a == b:
                table[a, b] = np.sum([1.0 / (nodes[a] - nodes[k]) for k in range(count) if k != a])
            else:
                table[a, b] = weights[a] / weights[b] / (nodes[a] - nodes[b])
    return [[float(np.float32(v)) for v in row] for row in table]


def dot4(coefs, terms):
    total = None
    for c, t in zip(coefs, terms):
        if c == 0.0:
            continue
        total = c * t if total is None else total + c * t
    return total


def kernel(
    faces, cols, nf, nbx, nby, R,
    fields_hbm, diag_ref, cross_ref, mass_ref, out_hbm,
    raw, U, M, W, T, rmass,
    sR1, sC1, sK1, rR1, rC1, rK1, sR2, sC2, sK2, rR2, rC2, rK2,
    load_sem, store_sem, send_sem, recv_sem,
):
    face, col = lax.axis_index("face"), lax.axis_index("col")
    fside = (lax.rem(face + faces - 1, faces), lax.rem(face + 1, faces))
    cside = (lax.rem(col + cols - 1, cols), lax.rem(col + 1, cols))
    peers = [(fside[0], col), (fside[1], col), (face, cside[0]), (face, cside[1])]
    peers += [(fside[s], cside[t]) for s in range(2) for t in range(2)]

    loads = [
        pltpu.make_async_copy(fields_hbm.at[f], raw.at[f], load_sem.at[f]) for f in range(nf)
    ]
    for load in loads:
        load.start()
    barrier = pltpu.get_barrier_semaphore()
    for peer in peers:
        pl.semaphore_signal(barrier, inc=1, device_id=peer, device_id_type=MESH)

    D = derivative_table()
    lanes = raw.shape[-1]
    n = nbx * nby
    nx, ny = 4 * nbx, 4 * nby
    lead = up8(nby + 1)

    row = lax.broadcasted_iota(jnp.int32, (16 * R, 1), 0)
    a_of = sum((row >= 4 * R * k).astype(jnp.int32) for k in range(1, 4))
    rest = row - 4 * R * a_of
    j_of = sum((rest >= R * k).astype(jnp.int32) for k in range(1, 4))
    r_of = rest - R * j_of
    ex_of = sum((r_of >= nby * k).astype(jnp.int32) for k in range(1, nbx))
    ey_of = r_of - nby * ex_of
    valid = r_of < n
    x_at = lax.broadcasted_iota(jnp.int32, (16 * R, nx), 1)
    y_at = lax.broadcasted_iota(jnp.int32, (16 * R, ny), 1)
    pick_x = jnp.where((x_at == 4 * ex_of + a_of) & valid, 1.0, 0.0).astype(jnp.bfloat16)
    keep_y = jnp.where(y_at == 4 * ey_of + j_of, 1.0, 0.0)
    ones = jnp.ones((ny, lanes), jnp.bfloat16)

    def planes(m):
        total = None
        for _ in range(3):
            part = m.astype(jnp.bfloat16)
            m = m - part.astype(jnp.float32)
            rows = jnp.dot(pick_x, part, preferred_element_type=jnp.float32) * keep_y
            wide = jnp.dot(rows.astype(jnp.bfloat16), ones, preferred_element_type=jnp.float32)
            total = wide if total is None else total + wide
        return total.reshape(4, 4, R, lanes)

    M[0] = planes(diag_ref[0])
    M[1] = planes(cross_ref[...])
    M[2] = planes(diag_ref[1])
    W[:, :, pl.ds(lead + nf * R, R), :] = planes(mass_ref[...])
    for at in (0, lead + (nf + 1) * R):
        W[:, :, pl.ds(at, lead), :] = jnp.zeros((4, 4, lead, lanes), jnp.float32)

    r_one = lax.broadcasted_iota(jnp.int32, (R, lanes), 0)
    ey_one = r_one - nby * sum((r_one >= nby * k).astype(jnp.int32) for k in range(1, nbx))
    inside = r_one < n
    low = jnp.where(inside & (ey_one > 0), 1.0, 0.0)
    high = jnp.where(inside & (ey_one < nby - 1), 1.0, 0.0)

    pad = n // 8 * 8
    for f in range(nf):
        for a in range(4):
            for j in range(4):
                U[a, j, pl.ds(f * R + pad, R - pad), :] = jnp.zeros((R - pad, lanes), jnp.float32)
    for f in range(nf):
        loads[f].wait()
        for ex in range(nbx):
            for a in range(4):
                for j in range(4):
                    U[a, j, pl.ds(f * R + nby * ex, nby), :] = raw[
                        f, 4 * ex + a, pl.ds(j, nby, stride=4), :
                    ]

    def laplace(f, carry):
        for rb in range(R // 8):
            at = pl.ds(pl.multiple_of(f * R + rb * 8, 8), 8)
            mat = pl.ds(rb * 8, 8)
            u = [[U[a, j, at, :] for j in range(4)] for a in range(4)]
            fx = [[None] * 4 for _ in range(4)]
            fy = [[None] * 4 for _ in range(4)]
            for a in range(4):
                for j in range(4):
                    gx = dot4(D[a], [u[b][j] for b in range(4)])
                    gy = dot4(D[j], [u[a][d] for d in range(4)])
                    m0, mc, m1 = M[0, a, j, mat, :], M[1, a, j, mat, :], M[2, a, j, mat, :]
                    fx[a][j] = m0 * gx + mc * gy
                    fy[a][j] = mc * gx + m1 * gy
            wat = pl.ds(pl.multiple_of(f * R + rb * 8 + lead, 8), 8)
            for a in range(4):
                for j in range(4):
                    W[a, j, wat, :] = dot4(
                        [-D[b][a] for b in range(4)], [fx[b][j] for b in range(4)]
                    ) + dot4([-D[d][j] for d in range(4)], [fy[a][d] for d in range(4)])
        return carry

    def partial_assemble(f):
        def w(a, j, shift):
            return W[a, j, pl.ds(lead + f * R + shift, R), :]

        def s(a, j, shift):
            if a == 0:
                return w(0, j, shift) + w(3, j, shift - nby)
            if a == 3:
                return w(3, j, shift) + w(0, j, shift + nby)
            return w(a, j, shift)

        at = pl.ds(f * R, R)
        for a in range(4):
            T[a, 0, at, :] = s(a, 0, 0) + low * s(a, 3, -1)
            T[a, 1, at, :] = s(a, 1, 0)
            T[a, 2, at, :] = s(a, 2, 0)
            T[a, 3, at, :] = s(a, 3, 0) + high * s(a, 0, 1)

    def exchange(phase, count, sR, sC, sK, rR, rC, rK):
        wx, wy = count * nby, count * nbx
        for d in range(2):
            e = 3 * d
            for f in range(count):
                for k in range(4):
                    sR[d, pl.ds(k * wx + f * nby, nby), :] = T[
                        e, k, pl.ds(f * R + d * (nbx - 1) * nby, nby), :
                    ]
                    sC[d, pl.ds(k * wy + f * nbx, nbx), :] = T[
                        k, e, pl.ds(f * R + d * (nby - 1), nbx, stride=nby), :
                    ]
        for s in range(2):
            for t in range(2):
                start = s * (nbx - 1) * nby + t * (nby - 1)
                for f in range(count):
                    sK[2 * s + t, pl.ds(f, 1), :] = T[3 * s, 3 * t, pl.ds(f * R + start, 1), :]
        pairs = [(sR.at[d], rR.at[1 - d]) for d in range(2)]
        pairs += [(sC.at[d], rC.at[1 - d]) for d in range(2)]
        pairs += [(sK.at[k], rK.at[3 - k]) for k in range(4)]
        copies = []
        for k, (src, dst) in enumerate(pairs):
            back = k ^ 1 if k < 4 else 11 - k
            copies.append(
                pltpu.make_async_remote_copy(
                    src_ref=src, dst_ref=dst,
                    send_sem=send_sem.at[phase, k], recv_sem=recv_sem.at[phase, back],
                    device_id=peers[k], device_id_type=MESH,
                )
            )
            copies[-1].start()
        return copies

    def finish(copies, count, rR, rC, rK):
        wx, wy = count * nby, count * nbx
        for copy in copies:
            copy.wait_recv()
        for d in range(2):
            e = 3 * d
            for f in range(count):
                for k in range(4):
                    at = pl.ds(f * R + d * (nbx - 1) * nby, nby)
                    T[e, k, at, :] = T[e, k, at, :] + rR[d, pl.ds(k * wx + f * nby, nby), :]
        for d in range(2):
            e = 3 * d
            for f in range(count):
                for k in range(4):
                    at = pl.ds(f * R + d * (nby - 1), nbx, stride=nby)
                    T[k, e, at, :] = T[k, e, at, :] + rC[d, pl.ds(k * wy + f * nbx, nbx), :]
        for s in range(2):
            for t in range(2):
                start = s * (nbx - 1) * nby + t * (nby - 1)
                for f in range(count):
                    at = pl.ds(f * R + start, 1)
                    T[3 * s, 3 * t, at, :] = (
                        T[3 * s, 3 * t, at, :] + rK[2 * s + t, pl.ds(f, 1), :]
                    )

    lax.fori_loop(0, nf, laplace, 0)
    for f in range(nf + 1):
        partial_assemble(f)
    pl.semaphore_wait(barrier, len(peers))
    first_copies = exchange(0, nf + 1, sR1, sC1, sK1, rR1, rC1, rK1)
    finish(first_copies, nf + 1, rR1, rC1, rK1)
    for a in range(4):
        for j in range(4):
            total = T[a, j, pl.ds(nf * R, R), :]
            scale = jnp.where(inside, 1.0 / jnp.where(inside, total, 1.0), 0.0)
            rmass[a, j] = scale
            for f in range(nf):
                U[a, j, pl.ds(f * R, R), :] = T[a, j, pl.ds(f * R, R), :] * scale

    lax.fori_loop(0, nf, laplace, 0)
    for f in range(nf):
        partial_assemble(f)
    second_copies = exchange(1, nf, sR2, sC2, sK2, rR2, rC2, rK2)
    finish(second_copies, nf, rR2, rC2, rK2)
    stores = []
    for f in range(nf):
        for ex in range(nbx):
            for a in range(4):
                for j in range(4):
                    raw[f, 4 * ex + a, pl.ds(j, nby, stride=4), :] = (
                        T[a, j, pl.ds(f * R + nby * ex, nby), :]
                        * rmass[a, j, pl.ds(nby * ex, nby), :]
                    )
        stores.append(pltpu.make_async_copy(raw.at[f], out_hbm.at[f], store_sem.at[f]))
        stores[-1].start()
    for copy in first_copies + second_copies:
        copy.wait_send()
    for store in stores:
        store.wait()


def up8(count):
    return -(-count // 8) * 8


def solution(mesh):
    faces, cols = mesh.shape["face"], mesh.shape["col"]

    def shards(fields, metric_diag, metric_cross, point_mass):
        nf, rows, width, lanes = fields.shape
        nbx, nby = rows // 4, width // 4
        R = up8(nbx * nby + nby + 1)
        f32 = jnp.float32

        def vmem(*shape):
            return pltpu.VMEM(shape, f32)

        def edges(count):
            return [
                vmem(2, up8(4 * count * nby), lanes),
                vmem(2, up8(4 * count * nbx), lanes),
                vmem(4, up8(count), lanes),
            ]

        return pl.pallas_call(
            functools.partial(kernel, faces, cols, nf, nbx, nby, R),
            out_shape=jax.ShapeDtypeStruct(fields.shape, f32),
            in_specs=[pl.BlockSpec(memory_space=pl.ANY)]
            + [pl.BlockSpec(memory_space=pltpu.VMEM)] * 3,
            out_specs=pl.BlockSpec(memory_space=pl.ANY),
            scratch_shapes=[
                vmem(nf, rows, width, lanes),
                vmem(4, 4, nf * R, lanes),
                vmem(3, 4, 4, R, lanes),
                vmem(4, 4, 2 * up8(nby + 1) + (nf + 1) * R, lanes),
                vmem(4, 4, (nf + 1) * R, lanes),
                vmem(4, 4, R, lanes),
                *edges(nf + 1), *edges(nf + 1), *edges(nf), *edges(nf),
                pltpu.SemaphoreType.DMA((nf,)),
                pltpu.SemaphoreType.DMA((nf,)),
                pltpu.SemaphoreType.DMA((2, 8)),
                pltpu.SemaphoreType.DMA((2, 8)),
            ],
            compiler_params=pltpu.CompilerParams(
                collective_id=0, has_side_effects=True, vmem_limit_bytes=32 * 1024 * 1024
            ),
        )(fields, metric_diag, metric_cross, point_mass)

    return jax.shard_map(
        shards,
        mesh=mesh,
        in_specs=(
            P(None, "face", "col", None),
            P(None, "face", "col"),
            P("face", "col"),
            P("face", "col"),
        ),
        out_specs=P(None, "face", "col", None),
        check_vma=False,
    )
```

```python
import functools

import jax
import jax.numpy as jnp
import numpy as np
from jax import lax
from jax.experimental import pallas as pl
from jax.experimental.pallas import tpu as pltpu
from jax.sharding import PartitionSpec as P

MESH = pl.DeviceIdType.MESH


def derivative_table():
    small = 1.0 / np.sqrt(5.0)
    nodes = np.array([-1.0, -small, small, 1.0])
    count = nodes.shape[0]
    weights = np.array(
        [np.prod([nodes[a] - nodes[k] for k in range(count) if k != a]) for a in range(count)]
    )
    table = np.zeros((count, count))
    for a in range(count):
        for b in range(count):
            if a == b:
                table[a, b] = np.sum([1.0 / (nodes[a] - nodes[k]) for k in range(count) if k != a])
            else:
                table[a, b] = weights[a] / weights[b] / (nodes[a] - nodes[b])
    return [[float(np.float32(v)) for v in row] for row in table]


def dot4(coefs, terms):
    total = None
    for c, t in zip(coefs, terms):
        if isinstance(c, float) and c == 0.0:
            continue
        total = c * t if total is None else total + c * t
    return total


def kernel(
    faces, cols, nf, nbx, nby,
    fields_hbm, diag_ref, cross_ref, mass_ref, out_ref,
    raw, U, M, W, T, spread, rM,
    sC1, rR1, rC1, rK1, sC2, rR2, rC2, rK2,
    load_sem, mass_send, mass_recv, send_sem, recv_sem,
):
    face, col = lax.axis_index("face"), lax.axis_index("col")
    fside = (lax.rem(face + faces - 1, faces), lax.rem(face + 1, faces))
    cside = (lax.rem(col + cols - 1, cols), lax.rem(col + 1, cols))
    peers = [(fside[0], col), (fside[1], col), (face, cside[0]), (face, cside[1])]
    peers += [(fside[s], cside[t]) for s in range(2) for t in range(2)]
    opposite = [1, 0, 3, 2, 7, 6, 5, 4]

    nx, ny, nq = 4 * nbx, 4 * nby, 2 * nby
    lanes = raw.shape[-1]
    order = [0, nbx - 1] + list(range(1, nbx - 1))
    loads = {
        ex: pltpu.make_async_copy(
            fields_hbm.at[pl.ds(4 * ex, 4)], raw.at[pl.ds(4 * ex, 4)], load_sem.at[ex]
        )
        for ex in order
    }
    for ex in order:
        loads[ex].start()
    barrier = pltpu.get_barrier_semaphore()
    for peer in peers:
        pl.semaphore_signal(barrier, inc=1, device_id=peer, device_id_type=MESH)

    D = derivative_table()
    sub = lax.broadcasted_iota(jnp.int32, (2 * nf, lanes), 0)
    is_low = sub < nf
    low = jnp.where(is_low, 1.0, 0.0)
    high = 1.0 - low

    def swap(v):
        return pltpu.roll(v, nf, 0)

    def halves(table):
        return [
            [
                jnp.where(is_low, table[2 * p][2 * q + k], table[2 * p + 1][2 * q + 1 - k])
                for q in range(2) for k in range(2)
            ]
            for p in range(2)
        ]

    minus_t = [[-D[b][a] for b in range(4)] for a in range(4)]
    D_half, minus_half = halves(D), halves(minus_t)

    row = lax.broadcasted_iota(jnp.int32, (nf * ny, 3 * ny), 0)
    lane = lax.broadcasted_iota(jnp.int32, (nf * ny, 3 * ny), 1)
    keep = jnp.zeros((nf * ny, 3 * ny), jnp.float32)
    for k in range(3):
        first_row = nf * (lane - k * ny)
        keep = jnp.where((row >= first_row) & (row < first_row + nf), 1.0, keep)
    ones = jnp.ones((3 * ny, lanes), jnp.bfloat16)

    def split(slot, m):
        parts = []
        for _ in range(3):
            part = m.astype(jnp.bfloat16).astype(jnp.float32)
            m = m - part
            parts.append(part)
        spread[slot] = jnp.concatenate(parts, axis=1)

    def spread_row(slot, x):
        left = (keep * spread[slot, pl.ds(x, 1), :]).astype(jnp.bfloat16)
        wide = jnp.dot(left, ones, preferred_element_type=jnp.float32)
        M[slot, x] = wide.reshape(nq, 2 * nf, lanes)

    split(0, diag_ref[0])
    split(1, cross_ref[...])
    split(2, diag_ref[1])
    for x in range(nx):
        for slot in range(3):
            spread_row(slot, x)

    def laplace(src, ex, ey):
        u = [[src[4 * ex + a, 2 * ey + p] for p in range(2)] for a in range(4)]
        fx = [[None] * 2 for _ in range(4)]
        fy = [[None] * 2 for _ in range(4)]
        for a in range(4):
            mix = [u[a][0], swap(u[a][0]), u[a][1], swap(u[a][1])]
            for p in range(2):
                at = (4 * ex + a, 2 * ey + p)
                gx = dot4(D[a], [u[b][p] for b in range(4)])
                gy = dot4(D_half[p], mix)
                m0, mc, m1 = M[(0,) + at], M[(1,) + at], M[(2,) + at]
                fx[a][p] = m0 * gx + mc * gy
                fy[a][p] = mc * gx + m1 * gy
        for a in range(4):
            mix = [fy[a][0], swap(fy[a][0]), fy[a][1], swap(fy[a][1])]
            for p in range(2):
                W[4 * ex + a, 2 * ey + p] = dot4(
                    minus_t[a], [fx[b][p] for b in range(4)]
                ) + dot4(minus_half[p], mix)

    def rows_sum(x, q):
        if x % 4 == 0 and x > 0:
            return W[x, q] + W[x - 1, q]
        if x % 4 == 3 and x < nx - 1:
            return W[x, q] + W[x + 1, q]
        return W[x, q]

    def assemble_row(x):
        line = [rows_sum(x, q) for q in range(nq)]
        for ey in range(1, nby):
            v, w = line[2 * ey - 1], line[2 * ey]
            line[2 * ey - 1], line[2 * ey] = v + high * swap(w), w + low * swap(v)
        for q in range(nq):
            T[x, q] = line[q]
            if x % 4 == 3 and x < nx - 1:
                T[x + 1, q] = line[q]

    def send(phase, k, src, dst):
        copy = pltpu.make_async_remote_copy(
            src_ref=src, dst_ref=dst,
            send_sem=send_sem.at[phase, k], recv_sem=recv_sem.at[phase, opposite[k]],
            device_id=peers[k], device_id_type=MESH,
        )
        copy.start()
        return copy

    def phase_sends(phase, src, sC, rR, rC, rK, ready):
        copies = [None] * 8
        for ex in order[:2]:
            ready(ex)
            for ey in range(nby):
                laplace(src, ex, ey)
        for x in (0, nx - 1):
            assemble_row(x)
        if phase == 0:
            pl.semaphore_wait(barrier, len(peers))
        for s in range(2):
            for t in range(2):
                k = 4 + 2 * s + t
                copies[k] = send(
                    phase, k, W.at[s * (nx - 1), t * (nq - 1)], rK.at[3 - 2 * s - t]
                )
        for s in range(2):
            copies[s] = send(phase, s, T.at[s * (nx - 1)], rR.at[1 - s])
        if phase == 0:
            for k in range(8):
                masses.append(
                    pltpu.make_async_remote_copy(
                        src_ref=mass_ref, dst_ref=rM.at[opposite[k]],
                        send_sem=mass_send.at[k], recv_sem=mass_recv.at[opposite[k]],
                        device_id=peers[k], device_id_type=MESH,
                    )
                )
                masses[-1].start()
        for ex in order[2:]:
            ready(ex)
            for ey in range(nby):
                laplace(src, ex, ey)
        for k in range(nx // 2):
            a, b = rows_sum(2 * k, 0), rows_sum(2 * k + 1, 0)
            sC[0, k] = jnp.where(is_low, a, swap(b))
            a, b = rows_sum(2 * k, nq - 1), rows_sum(2 * k + 1, nq - 1)
            sC[1, k] = jnp.where(is_low, swap(a), b)
        for t in range(2):
            copies[2 + t] = send(phase, 2 + t, sC.at[t], rC.at[1 - t])
        for x in range(1, nx - 1):
            if x % 4 != 0:
                assemble_row(x)
        return copies

    def finished(x, rR, rC, rK):
        line = [T[x, q] for q in range(nq)]
        if x in (0, nx - 1):
            s = 0 if x == 0 else 1
            line = [v + rR[s, q] for q, v in enumerate(line)]
            line[0] = line[0] + low * swap(rK[2 * s])
            line[-1] = line[-1] + high * swap(rK[2 * s + 1])
        before, after = rC[0, x // 2], rC[1, x // 2]
        if x % 2 == 0:
            after = swap(after)
        else:
            before = swap(before)
        line[0] = line[0] + low * before
        line[-1] = line[-1] + high * after
        return line

    masses = []
    first_copies = phase_sends(0, raw, sC1, rR1, rC1, rK1, lambda ex: loads[ex].wait())

    for copy in masses:
        copy.wait_recv()
    x_at = lax.broadcasted_iota(jnp.int32, (nx, ny), 0)
    y_at = lax.broadcasted_iota(jnp.int32, (nx, ny), 1)
    x_low, x_high = (x_at & 3) == 0, (x_at & 3) == 3
    y_low, y_high = (y_at & 3) == 0, (y_at & 3) == 3

    def mass_rows(own, prev, nxt):
        down = jnp.concatenate([prev[nx - 1:], own[: nx - 1]], axis=0)
        up = jnp.concatenate([own[1:], nxt[:1]], axis=0)
        return own + jnp.where(x_low, down, 0.0) + jnp.where(x_high, up, 0.0)

    here = mass_rows(mass_ref[...], rM[0], rM[1])
    left = mass_rows(rM[2], rM[4], rM[6])
    right = mass_rows(rM[3], rM[5], rM[7])
    back = jnp.concatenate([left[:, ny - 1:], here[:, : ny - 1]], axis=1)
    ahead = jnp.concatenate([here[:, 1:], right[:, :1]], axis=1)
    mass_sum = here + jnp.where(y_low, back, 0.0) + jnp.where(y_high, ahead, 0.0)
    split(3, 1.0 / mass_sum)
    for x in range(nx):
        spread_row(3, x)

    for copy in first_copies:
        copy.wait_recv()
    for x in range(nx):
        line = finished(x, rR1, rC1, rK1)
        for q in range(nq):
            U[x, q] = line[q] * M[3, x, q]
    for copy in first_copies:
        copy.wait_send()

    second_copies = phase_sends(1, U, sC2, rR2, rC2, rK2, lambda ex: None)
    for copy in second_copies:
        copy.wait_recv()
    for x in range(nx):
        line = finished(x, rR2, rC2, rK2)
        for q in range(nq):
            out_ref[x, q] = line[q] * M[3, x, q]
    for copy in second_copies + masses:
        copy.wait_send()


def solution(mesh):
    faces, cols = mesh.shape["face"], mesh.shape["col"]

    def shards(fields, metric_diag, metric_cross, point_mass):
        nf, nx, ny, lanes = fields.shape
        nbx, nby = nx // 4, ny // 4
        f32 = jnp.float32
        tiles = (nx, ny // 2, 2 * nf, lanes)

        def vmem(*shape):
            return pltpu.VMEM(shape, f32)

        def landing():
            return [
                vmem(2, nx // 2, 2 * nf, lanes),
                vmem(2, ny // 2, 2 * nf, lanes),
                vmem(2, nx // 2, 2 * nf, lanes),
                vmem(4, 2 * nf, lanes),
            ]

        out = pl.pallas_call(
            functools.partial(kernel, faces, cols, nf, nbx, nby),
            out_shape=jax.ShapeDtypeStruct(tiles, f32),
            in_specs=[pl.BlockSpec(memory_space=pl.ANY)]
            + [pl.BlockSpec(memory_space=pltpu.VMEM)] * 3,
            out_specs=pl.BlockSpec(memory_space=pltpu.VMEM),
            scratch_shapes=[
                vmem(*tiles),
                vmem(*tiles),
                vmem(4, *tiles),
                vmem(*tiles),
                vmem(*tiles),
                vmem(4, nx, 3 * ny),
                vmem(8, nx, ny),
                *landing(), *landing(),
                pltpu.SemaphoreType.DMA((nbx,)),
                pltpu.SemaphoreType.DMA((8,)),
                pltpu.SemaphoreType.DMA((8,)),
                pltpu.SemaphoreType.DMA((2, 8)),
                pltpu.SemaphoreType.DMA((2, 8)),
            ],
            compiler_params=pltpu.CompilerParams(
                collective_id=0, has_side_effects=True, vmem_limit_bytes=32 * 1024 * 1024
            ),
        )(
            fields.transpose(1, 2, 0, 3).reshape(tiles),
            metric_diag, metric_cross, point_mass,
        )
        return out.reshape(nx, ny, nf, lanes).transpose(2, 0, 1, 3)

    return jax.shard_map(
        shards,
        mesh=mesh,
        in_specs=(
            P(None, "face", "col", None),
            P(None, "face", "col"),
            P("face", "col"),
            P("face", "col"),
        ),
        out_specs=P(None, "face", "col", None),
        check_vma=False,
    )
```

```python
import functools

import jax
import jax.numpy as jnp
import numpy as np
from jax import lax
from jax.experimental import pallas as pl
from jax.experimental.pallas import tpu as pltpu
from jax.sharding import PartitionSpec as P

MESH = pl.DeviceIdType.MESH


def derivative_table():
    small = 1.0 / np.sqrt(5.0)
    nodes = np.array([-1.0, -small, small, 1.0])
    count = nodes.shape[0]
    weights = np.array(
        [np.prod([nodes[a] - nodes[k] for k in range(count) if k != a]) for a in range(count)]
    )
    table = np.zeros((count, count))
    for a in range(count):
        for b in range(count):
            if a == b:
                table[a, b] = np.sum([1.0 / (nodes[a] - nodes[k]) for k in range(count) if k != a])
            else:
                table[a, b] = weights[a] / weights[b] / (nodes[a] - nodes[b])
    return [[float(np.float32(v)) for v in row] for row in table]


def dot4(coefs, terms):
    total = None
    for c, t in zip(coefs, terms):
        if isinstance(c, float) and c == 0.0:
            continue
        total = c * t if total is None else total + c * t
    return total


def kernel(
    faces, cols, nf, nbx, nby,
    fields_hbm, diag_ref, cross_ref, mass_ref, out_ref,
    raw, U, M, W, T, spread, sM, rM,
    sC1, sK1, rR1, rC1, rK1, sC2, sK2, rR2, rC2, rK2,
    load_sem, mass_send, mass_recv, send_sem, recv_sem,
):
    face, col = lax.axis_index("face"), lax.axis_index("col")
    fside = (lax.rem(face + faces - 1, faces), lax.rem(face + 1, faces))
    cside = (lax.rem(col + cols - 1, cols), lax.rem(col + 1, cols))
    peers = [(fside[0], col), (fside[1], col), (face, cside[0]), (face, cside[1])]
    peers += [(fside[s], cside[t]) for s in range(2) for t in range(2)]
    opposite = [1, 0, 3, 2, 7, 6, 5, 4]

    nx, ny, nq = 4 * nbx, 4 * nby, 2 * nby
    lanes = raw.shape[-1]
    order = [0, nbx - 1] + list(range(1, nbx - 1))
    loads = {
        ex: pltpu.make_async_copy(
            fields_hbm.at[pl.ds(4 * ex, 4)], raw.at[pl.ds(4 * ex, 4)], load_sem.at[ex]
        )
        for ex in order
    }
    for ex in order:
        loads[ex].start()
    barrier = pltpu.get_barrier_semaphore()
    for peer in peers:
        pl.semaphore_signal(barrier, inc=1, device_id=peer, device_id_type=MESH)

    square_x = lax.broadcasted_iota(jnp.int32, (nx, nx), 0)
    square_y = lax.broadcasted_iota(jnp.int32, (nx, nx), 1)
    diagonal = square_x == square_y
    sM[pl.ds(0, 1), pl.ds(0, ny)] = mass_ref[pl.ds(0, 1), :]
    sM[pl.ds(1, 1), pl.ds(0, ny)] = mass_ref[pl.ds(nx - 1, 1), :]
    for t in range(2):
        column = mass_ref[:, pl.ds(t * (ny - 1), 1)]
        sM[pl.ds(2 + t, 1), pl.ds(0, nx)] = jnp.sum(
            jnp.where(diagonal, column, 0.0), axis=0, keepdims=True
        )

    D = derivative_table()
    sub = lax.broadcasted_iota(jnp.int32, (2 * nf, lanes), 0)
    is_low = sub < nf
    low = jnp.where(is_low, 1.0, 0.0)
    high = 1.0 - low

    def swap(v):
        return pltpu.roll(v, nf, 0)

    def halves(table):
        return [
            [
                jnp.where(is_low, table[2 * p][2 * q + k], table[2 * p + 1][2 * q + 1 - k])
                for q in range(2) for k in range(2)
            ]
            for p in range(2)
        ]

    minus_t = [[-D[b][a] for b in range(4)] for a in range(4)]
    D_half, minus_half = halves(D), halves(minus_t)

    row = lax.broadcasted_iota(jnp.int32, (nf * ny, 3 * ny), 0)
    lane = lax.broadcasted_iota(jnp.int32, (nf * ny, 3 * ny), 1)
    keep = jnp.zeros((nf * ny, 3 * ny), jnp.float32)
    for k in range(3):
        first_row = nf * (lane - k * ny)
        keep = jnp.where((row >= first_row) & (row < first_row + nf), 1.0, keep)
    ones = jnp.ones((3 * ny, lanes), jnp.bfloat16)

    def split(slot, m):
        parts = []
        for _ in range(3):
            part = m.astype(jnp.bfloat16).astype(jnp.float32)
            m = m - part
            parts.append(part)
        spread[slot] = jnp.concatenate(parts, axis=1)

    def spread_row(slot, x):
        left = (keep * spread[slot, pl.ds(x, 1), :]).astype(jnp.bfloat16)
        wide = jnp.dot(left, ones, preferred_element_type=jnp.float32)
        M[slot, x] = wide.reshape(nq, 2 * nf, lanes)

    split(0, diag_ref[:, 0, :])
    split(1, cross_ref[...])
    split(2, diag_ref[:, 1, :])
    def spread_metrics(x, carry):
        for slot in range(3):
            spread_row(slot, x)
        return carry

    lax.fori_loop(0, nx, spread_metrics, 0)

    def laplace(src, ex, ey):
        u = [[src[4 * ex + a, 2 * ey + p] for p in range(2)] for a in range(4)]
        fx = [[None] * 2 for _ in range(4)]
        fy = [[None] * 2 for _ in range(4)]
        for a in range(4):
            mix = [u[a][0], swap(u[a][0]), u[a][1], swap(u[a][1])]
            for p in range(2):
                at = (4 * ex + a, 2 * ey + p)
                gx = dot4(D[a], [u[b][p] for b in range(4)])
                gy = dot4(D_half[p], mix)
                m0, mc, m1 = M[(0,) + at], M[(1,) + at], M[(2,) + at]
                fx[a][p] = m0 * gx + mc * gy
                fy[a][p] = mc * gx + m1 * gy
        for a in range(4):
            mix = [fy[a][0], swap(fy[a][0]), fy[a][1], swap(fy[a][1])]
            for p in range(2):
                W[4 * ex + a, 2 * ey + p] = dot4(
                    minus_t[a], [fx[b][p] for b in range(4)]
                ) + dot4(minus_half[p], mix)

    def rows_sum(x, q):
        if x % 4 == 0 and x > 0:
            return W[x, q] + W[x - 1, q]
        if x % 4 == 3 and x < nx - 1:
            return W[x, q] + W[x + 1, q]
        return W[x, q]

    def assemble_row(x):
        line = [rows_sum(x, q) for q in range(nq)]
        for ey in range(1, nby):
            v, w = line[2 * ey - 1], line[2 * ey]
            line[2 * ey - 1], line[2 * ey] = v + high * swap(w), w + low * swap(v)
        for q in range(nq):
            T[x, q] = line[q]
            if x % 4 == 3 and x < nx - 1:
                T[x + 1, q] = line[q]

    def send(phase, k, src, dst):
        copy = pltpu.make_async_remote_copy(
            src_ref=src, dst_ref=dst,
            send_sem=send_sem.at[phase, k], recv_sem=recv_sem.at[phase, opposite[k]],
            device_id=peers[k], device_id_type=MESH,
        )
        copy.start()
        return copy

    def corner(s, t):
        tile = W[s * (nx - 1), t * (nq - 1)]
        return tile[t * nf:(t + 1) * nf]

    def lap_rows(src, first, last):
        def one(i, carry):
            laplace(src, first + lax.div(i, nby), lax.rem(i, nby))
            return carry

        lax.fori_loop(0, (last - first) * nby, one, 0)

    def phase_sends(phase, src, sC, sK, rR, rC, rK, ready):
        copies = [None] * 8
        for s, ex in enumerate(order[:2]):
            ready(ex)
            lap_rows(src, ex, ex + 1)
            assemble_row(s * (nx - 1))
            for t in range(2):
                sK[2 * s + t] = corner(s, t)
            if phase == 0 and s == 0:
                pl.semaphore_wait(barrier, len(peers))
            copies[s] = send(phase, s, T.at[s * (nx - 1)], rR.at[1 - s])
            for t in range(2):
                k = 2 * s + t
                copies[4 + k] = send(phase, 4 + k, sK.at[k], rK.at[3 - k])
        if phase == 0:
            for k in range(8):
                masses.append(
                    pltpu.make_async_remote_copy(
                        src_ref=sM, dst_ref=rM.at[opposite[k]],
                        send_sem=mass_send.at[k], recv_sem=mass_recv.at[opposite[k]],
                        device_id=peers[k], device_id_type=MESH,
                    )
                )
                masses[-1].start()
        for ex in order[2:]:
            ready(ex)
        lap_rows(src, 1, nbx - 1)
        for k in range(nx // 2):
            a, b = rows_sum(2 * k, 0), rows_sum(2 * k + 1, 0)
            sC[0, k] = jnp.where(is_low, a, swap(b))
            a, b = rows_sum(2 * k, nq - 1), rows_sum(2 * k + 1, nq - 1)
            sC[1, k] = jnp.where(is_low, swap(a), b)
        for t in range(2):
            copies[2 + t] = send(phase, 2 + t, sC.at[t], rC.at[1 - t])
        for x in range(1, nx - 1):
            if x % 4 != 0:
                assemble_row(x)
        return copies

    def finished(x, rR, rC, rK, out, done):
        scale = lambda q, v: v * M[3, x, q]
        for q in range(1, nq - 1):
            if done(x, q):
                continue
            v = T[x, q]
            if x in (0, nx - 1):
                v = v + rR[0 if x == 0 else 1, q]
            out[x, q] = scale(q, v)
        ends = [T[x, 0], T[x, nq - 1]]
        before, after = rC[0, x // 2], rC[1, x // 2]
        if x % 2 == 0:
            after = swap(after)
        else:
            before = swap(before)
        ends = [ends[0] + low * before, ends[1] + high * after]
        if x in (0, nx - 1):
            s = 0 if x == 0 else 1
            zero = jnp.zeros((nf, lanes), jnp.float32)
            ends[0] = ends[0] + rR[s, 0] + jnp.concatenate([rK[2 * s], zero], axis=0)
            ends[1] = ends[1] + rR[s, nq - 1] + jnp.concatenate([zero, rK[2 * s + 1]], axis=0)
        out[x, 0] = scale(0, ends[0])
        out[x, nq - 1] = scale(nq - 1, ends[1])

    masses = []

    first_copies = phase_sends(
        0, raw, sC1, sK1, rR1, rC1, rK1, lambda ex: loads[ex].wait()
    )

    for copy in masses:
        copy.wait_recv()
    x_at = lax.broadcasted_iota(jnp.int32, (nx, ny), 0)
    y_at = lax.broadcasted_iota(jnp.int32, (nx, ny), 1)
    x_low, x_high = (x_at & 3) == 0, (x_at & 3) == 3
    y_low, y_high = (y_at & 3) == 0, (y_at & 3) == 3

    def edge_row(k, s):
        return rM[k, pl.ds(s, 1), pl.ds(0, ny)]

    def edge_column(k, t):
        return jnp.sum(
            jnp.where(diagonal, rM[k, pl.ds(2 + t, 1), pl.ds(0, nx)], 0.0), axis=1, keepdims=True
        )

    def mass_rows(own, prev, nxt, below, above):
        down = jnp.concatenate([prev, own[: nx - 1]], axis=0)
        up = jnp.concatenate([own[1:], nxt], axis=0)
        return own + jnp.where(below, down, 0.0) + jnp.where(above, up, 0.0)

    here = mass_rows(mass_ref[...], edge_row(0, 1), edge_row(1, 0), x_low, x_high)

    def beside(k, t):
        before = edge_row(4 + k, 1)[:, t * (ny - 1):t * (ny - 1) + 1]
        after = edge_row(6 + k, 0)[:, t * (ny - 1):t * (ny - 1) + 1]
        return mass_rows(edge_column(2 + k, t), before, after, x_low[:, :1], x_high[:, :1])

    back = jnp.concatenate([beside(0, 1), here[:, : ny - 1]], axis=1)
    ahead = jnp.concatenate([here[:, 1:], beside(1, 0)], axis=1)
    mass_sum = here + jnp.where(y_low, back, 0.0) + jnp.where(y_high, ahead, 0.0)
    split(3, 1.0 / mass_sum)
    def spread_mass(x, carry):
        spread_row(3, x)
        return carry

    lax.fori_loop(0, nx, spread_mass, 0)

    for copy in first_copies:
        copy.wait_recv()
    for x in range(nx):
        finished(x, rR1, rC1, rK1, U, lambda x, q: False)
    for copy in first_copies:
        copy.wait_send()

    second_copies = phase_sends(1, U, sC2, sK2, rR2, rC2, rK2, lambda ex: None)
    for x in range(1, nx - 1):
        for q in range(1, nq - 1):
            out_ref[x, q] = T[x, q] * M[3, x, q]
    for copy in second_copies:
        copy.wait_recv()
    for x in range(nx):
        finished(x, rR2, rC2, rK2, out_ref, lambda x, q: 0 < x < nx - 1)
    for copy in second_copies + masses:
        copy.wait_send()


def solution(mesh):
    faces, cols = mesh.shape["face"], mesh.shape["col"]

    def shards(fields, metric_diag, metric_cross, point_mass):
        nf, nx, ny, lanes = fields.shape
        nbx, nby = nx // 4, ny // 4
        f32 = jnp.float32
        tiles = (nx, ny // 2, 2 * nf, lanes)

        def vmem(*shape):
            return pltpu.VMEM(shape, f32)

        def landing():
            return [
                vmem(2, nx // 2, 2 * nf, lanes),
                vmem(4, nf, lanes),
                vmem(2, ny // 2, 2 * nf, lanes),
                vmem(2, nx // 2, 2 * nf, lanes),
                vmem(4, nf, lanes),
            ]

        out = pl.pallas_call(
            functools.partial(kernel, faces, cols, nf, nbx, nby),
            out_shape=jax.ShapeDtypeStruct(tiles, f32),
            in_specs=[pl.BlockSpec(memory_space=pltpu.HBM)]
            + [pl.BlockSpec(memory_space=pltpu.VMEM)] * 3,
            out_specs=pl.BlockSpec(memory_space=pltpu.VMEM),
            scratch_shapes=[
                vmem(*tiles),
                vmem(*tiles),
                vmem(4, *tiles),
                vmem(*tiles),
                vmem(*tiles),
                vmem(4, nx, 3 * ny),
                vmem(4, 128),
                vmem(8, 4, 128),
                *landing(), *landing(),
                pltpu.SemaphoreType.DMA((nbx,)),
                pltpu.SemaphoreType.DMA((8,)),
                pltpu.SemaphoreType.DMA((8,)),
                pltpu.SemaphoreType.DMA((2, 8)),
                pltpu.SemaphoreType.DMA((2, 8)),
            ],
            compiler_params=pltpu.CompilerParams(
                collective_id=0, has_side_effects=True, vmem_limit_bytes=66800000
            ),
        )(
            fields.transpose(1, 2, 0, 3).reshape(tiles),
            metric_diag.transpose(1, 0, 2), metric_cross, point_mass,
        )
        return out.reshape(nx, ny, nf, lanes).transpose(2, 0, 1, 3)

    return jax.shard_map(
        shards,
        mesh=mesh,
        in_specs=(
            P(None, "face", "col", None),
            P(None, "face", "col"),
            P("face", "col"),
            P("face", "col"),
        ),
        out_specs=P(None, "face", "col", None),
        check_vma=False,
    )
```
